32 devices in a mesh: section: 4 (over z), expert: 8 (over y, x, core).
Axes of the slice: x: 2, y: 2, z: 4, core: 2. Of those that a mesh axis runs over, the one named last changes fastest.
Arguments:
- act_a: bfloat16 [4, 512, 3584], P('section', 'expert'), may hold values from -6 to 6
- act_b: bfloat16 [4, 512, 3584], P('section', 'expert'), may hold values from -6 to 6
- grad_b: bfloat16 [4, 512, 3584], P('section', 'expert'), may hold values from -6 to 6
- ids_a: int32 [4, 512, 2], P('section', 'expert'), may hold values from 0 to 3, all different within a row; in each aligned block of 64 rows (0 to 63, 64 to 127, ..., all dimensions but the last counted through in order) at most 48 rows name the same one
- ids_b: int32 [4, 512, 2], P('section', 'expert'), may hold values from 0 to 3, all different within a row; in each aligned block of 64 rows (0 to 63, 64 to 127, ..., all dimensions but the last counted through in order) at most 48 rows name the same one
- scores_a: float32 [4, 512, 2], P('section', 'expert'), may hold values from 0.1 to 1
- scores_b: float32 [4, 512, 2], P('section', 'expert'), may hold values from 0.1 to 1
- w_gate: bfloat16 [4, 8, 3584, 512], P('section', 'expert'), may hold values from -0.09375 to 0.09375
- w_up: bfloat16 [4, 8, 3584, 512], P('section', 'expert'), may hold values from -0.09375 to 0.09375
- w_down: bfloat16 [4, 8, 512, 3584], P('section', 'expert'), may hold values from -0.1875 to 0.1875
Outputs:
- out_a: bfloat16 [4, 512, 3584], P('section', 'expert')
- grad_in_b: bfloat16 [4, 512, 3584], P('section', 'expert')
The draws below stay inside these ranges and needn't reach their ends.
Inputs may be any that keep to these rules, and one draw needn't show every extreme that they name: `ids_a`: each row names 2 different experts. Within the 64 rows of one device no expert is named by more than 48 rows, and in some device's rows some expert is named by exactly 48. `ids_b`: as for ids_a.
All inputs are finite; a program needn't handle non-finite values.
Results may differ from the reference program's by a relative error of at most 0.0072.
Values may be sent and summed in bfloat16 or wider, within the bound.
No kernel may reach another device: no remote copies, remote signals or barrier semaphores. Data moves between devices by JAX's collectives and lax.ppermute only.
A program may use at most 128 MiB of HBM per device.

```python
import math
import jax
import jax.numpy as jnp
import numpy as np
from jax import lax

D = 3584
FF = 1024
TOP = 2
TOK_DEV = 64
EXPERTS = 4
CAP = 48
TOKENS = 512
N_SECTION = 4
N_EXPERT = 8


def block_scale(key, shape, split, smallest, largest):
    gain = 1.0
    for dim, parts in split:
        draws = jax.random.uniform(jax.random.fold_in(jax.random.fold_in(key, 6), dim), (parts,), jnp.float32, smallest / len(split), largest / len(split))
        gain = gain * jnp.repeat(jnp.exp(draws), shape[dim] // parts).reshape((-1,) + (1,) * (len(shape) - 1 - dim))
    return gain


def assign_block(key, own, number, rows, number_of, top, limit, skew):
    ranking = jax.random.permutation(key, number_of)
    packed, common = shares(number_of, rows * top, limit, skew, True), shares(number_of, rows * top, limit, skew, False)
    places = jnp.arange(number_of)

    def named(sizes, offset_by):
        used = int((sizes > 0).sum())
        fixed = max(1, used // 4)
        moved = fixed + (places - fixed + offset_by * (used - fixed)) % max(1, number_of - fixed)
        return jnp.zeros((number_of,), jnp.int32).at[ranking[jnp.where(places < fixed, places, moved)]].set(jnp.asarray(sizes, jnp.int32))

    sizes = jnp.where(number % 4 == 0, named(packed, number // 4), named(common, number - number // 4 - 1))
    mixed = jax.random.permutation(jax.random.fold_in(own, 3), number_of)
    donor, taker = mixed[0:number_of // 2 * 2:2], mixed[1:number_of // 2 * 2:2]
    slack = jnp.minimum(sizes[donor] - 1, limit - sizes[taker]) // 2
    slack = jnp.where((donor == ranking[0]) | (taker == ranking[0]) | (sizes[taker] == 0), 0, jnp.maximum(slack, 0))
    moved = jax.random.randint(jax.random.fold_in(own, 4), (number_of // 2,), 0, 1 << 20) % (slack + 1)
    sizes = sizes.at[donor].add(-moved).at[taker].add(moved)
    members = jnp.searchsorted(jnp.cumsum(sizes), jnp.arange(rows * top), side="right").astype(jnp.int32)
    table = members.reshape(top, rows).T
    table = table[jax.random.permutation(jax.random.fold_in(own, 1), rows)]
    offset_by = jax.random.randint(jax.random.fold_in(own, 2), (rows, 1), 0, top)
    return jnp.take_along_axis(table, (jnp.arange(top)[None, :] + offset_by) % top, axis=1)


def shares(count, total, most, lean, full):
    loads = [(1 << 20) // math.isqrt(grade ** lean) + 1 for grade in range(1, count + 1)]
    largest = most if full else min(most, max(-(-total // count), total * loads[0] // sum(loads)))
    least = 1 if total - largest >= count - 1 else 0
    counts, rest = [largest] + [least] * (count - 1), total - largest - least * (count - 1)
    while rest > 0:
        movable = [i for i in range(1, count) if counts[i] < largest] or [i for i in range(1, count) if counts[i] < most]
        mass, remaining = sum([loads[i] for i in movable]), rest
        for i in movable:
            more = min(most - counts[i], max(1, remaining * loads[i] // mass), rest)
            counts[i] = counts[i] + more
            rest = rest - more
    return np.array(counts)


def centred(own_key, shape, deviation, reach, split=(), held_as=jnp.bfloat16):
    entries = deviation * jax.random.normal(own_key, shape, jnp.float32)
    if split:
        entries = entries * block_scale(own_key, shape, split, -0.22, 0.18)
    return jnp.clip(entries, -reach, reach).astype(held_as)


def setup_inputs(seed: int = 0) -> dict:
    streams_of = jax.random.split(jax.random.key(seed), 11)
    act_a = centred(streams_of[0], (N_SECTION, TOKENS, D), 1.0, 6.0, ((0, 4), (1, 8)))
    act_b = centred(streams_of[1], (N_SECTION, TOKENS, D), 1.0, 6.0, ((0, 4), (1, 8)))
    grad_b = centred(streams_of[2], (N_SECTION, TOKENS, D), 1.0, 6.0, ((0, 4), (1, 8)))
    ids_a_keys = jax.random.split(jax.random.fold_in(streams_of[3], 1), N_SECTION * TOKENS // TOK_DEV)
    ids_a_turns = jax.random.permutation(jax.random.fold_in(streams_of[3], 3), N_SECTION * TOKENS // TOK_DEV)
    ids_a = jax.vmap(lambda own, number: assign_block(jax.random.fold_in(streams_of[3], 2), own, number, TOK_DEV, EXPERTS, TOP, CAP, 2))(ids_a_keys, ids_a_turns).reshape((N_SECTION, TOKENS, TOP))
    ids_b_keys = jax.random.split(jax.random.fold_in(streams_of[4], 1), N_SECTION * TOKENS // TOK_DEV)
    ids_b_turns = jax.random.permutation(jax.random.fold_in(streams_of[4], 3), N_SECTION * TOKENS // TOK_DEV)
    ids_b = jax.vmap(lambda own, number: assign_block(jax.random.fold_in(streams_of[4], 2), own, number, TOK_DEV, EXPERTS, TOP, CAP, 2))(ids_b_keys, ids_b_turns).reshape((N_SECTION, TOKENS, TOP))
    scores_a = jnp.clip(jnp.exp(math.log(1.0) - 2.3025851 * jax.random.uniform(streams_of[5], (N_SECTION, TOKENS, TOP), jnp.float32) ** block_scale(streams_of[5], (N_SECTION, TOKENS, TOP), ((0, 4), (1, 8)), -0.2, 0.2)), 0.1, 1.0)
    scores_b = jnp.clip(jnp.exp(math.log(1.0) - 2.3025851 * jax.random.uniform(streams_of[6], (N_SECTION, TOKENS, TOP), jnp.float32) ** block_scale(streams_of[6], (N_SECTION, TOKENS, TOP), ((0, 4), (1, 8)), -0.2, 0.2)), 0.1, 1.0)
    w_gate = centred(streams_of[7], (N_SECTION, N_EXPERT, D, FF // 2), D ** -0.5, 0.09375, ((0, 4), (1, 8)))
    w_up = centred(streams_of[8], (N_SECTION, N_EXPERT, D, FF // 2), D ** -0.5, 0.09375, ((0, 4), (1, 8)))
    w_down = centred(streams_of[9], (N_SECTION, N_EXPERT, FF // 2, D), FF ** -0.5, 0.1875, ((0, 4), (1, 8)))
    return dict(act_a=act_a, act_b=act_b, grad_b=grad_b, ids_a=ids_a, ids_b=ids_b, scores_a=scores_a, scores_b=scores_b, w_gate=w_gate, w_up=w_up, w_down=w_down)


def make_place(ids):
    flat = ids.reshape(-1).astype(jnp.int32)
    onehot = (flat[:, None] == jnp.arange(EXPERTS, dtype=jnp.int32)[None, :]).astype(jnp.int32)
    before = (jnp.cumsum(onehot, 0).astype(jnp.int32) - onehot) * onehot
    slot = jnp.sum(before, 1).astype(jnp.int32)
    target = flat * CAP + slot
    return (target[:, None] == jnp.arange(EXPERTS * CAP, dtype=jnp.int32)[None, :]).astype(jnp.bfloat16)


def gate_weights(scores):
    return scores / jnp.sum(scores, -1, keepdims=True)


def scatter_rows(place, rows):
    return jnp.dot(place.T, rows, preferred_element_type=jnp.float32).astype(jnp.bfloat16)


def to_experts(bufs):
    grid = bufs.reshape(N_EXPERT, EXPERTS, CAP, D).transpose(1, 0, 2, 3)
    return grid.reshape(EXPERTS, N_EXPERT * CAP, D)


def from_experts(outs):
    grid = outs.reshape(EXPERTS, N_EXPERT, CAP, D).transpose(1, 0, 2, 3)
    return grid.reshape(N_EXPERT, EXPERTS * CAP, D)


def forward_half(rows, gate_w, up_w, down_w):
    first = jnp.dot(rows, gate_w, preferred_element_type=jnp.float32)
    second = jnp.dot(rows, up_w, preferred_element_type=jnp.float32)
    hidden = (jax.nn.silu(first) * second).astype(jnp.bfloat16)
    return jnp.dot(hidden, down_w, preferred_element_type=jnp.float32).astype(jnp.bfloat16)


def backward_half(rows, grads, gate_w, up_w, down_w):
    first = jnp.dot(rows, gate_w, preferred_element_type=jnp.float32)
    second = jnp.dot(rows, up_w, preferred_element_type=jnp.float32)
    dact = jnp.dot(grads, down_w.T, preferred_element_type=jnp.float32)
    sig = jax.nn.sigmoid(first)
    dfirst = (dact * second * sig * (1.0 + first * (1.0 - sig))).astype(jnp.bfloat16)
    dsecond = (dact * first * sig).astype(jnp.bfloat16)
    total = jnp.dot(dfirst, gate_w.T, preferred_element_type=jnp.float32)
    total = total + jnp.dot(dsecond, up_w.T, preferred_element_type=jnp.float32)
    return total.astype(jnp.bfloat16)


def section_forward(args):
    x, ids, scores, gate_w, up_w, down_w = args
    places = jax.vmap(make_place)(ids.reshape(N_EXPERT, TOK_DEV, TOP))
    xrep = jnp.repeat(x.reshape(N_EXPERT, TOK_DEV, D), TOP, axis=1)
    bufs = jax.vmap(scatter_rows)(places, xrep)
    rows = to_experts(bufs)
    gate2 = gate_w.reshape(EXPERTS, 2, D, FF // 2)
    up2 = up_w.reshape(EXPERTS, 2, D, FF // 2)
    down2 = down_w.reshape(EXPERTS, 2, FF // 2, D)

    def expert(item):
        r, g, u, v = item
        p0 = forward_half(r, g[0], u[0], v[0]).astype(jnp.float32)
        p1 = forward_half(r, g[1], u[1], v[1]).astype(jnp.float32)
        return (p0 + p1).astype(jnp.bfloat16)

    outs = lax.map(expert, (rows, gate2, up2, down2))
    back = from_experts(outs)
    weights = gate_weights(scores.reshape(N_EXPERT, TOK_DEV, TOP))

    def combine(place, buf, wts):
        picked = jnp.dot(place, buf, preferred_element_type=jnp.float32).reshape(TOK_DEV, TOP, D)
        return jnp.sum(wts[:, :, None] * picked, 1).astype(jnp.bfloat16)

    return jax.vmap(combine)(places, back, weights).reshape(TOKENS, D)


def section_backward(args):
    x, g, ids, scores, gate_w, up_w, down_w = args
    places = jax.vmap(make_place)(ids.reshape(N_EXPERT, TOK_DEV, TOP))
    weights = gate_weights(scores.reshape(N_EXPERT, TOK_DEV, TOP))
    xrep = jnp.repeat(x.reshape(N_EXPERT, TOK_DEV, D), TOP, axis=1)
    grep = (weights[:, :, :, None] * g.reshape(N_EXPERT, TOK_DEV, 1, D).astype(jnp.float32)).astype(jnp.bfloat16)
    grep = grep.reshape(N_EXPERT, TOK_DEV * TOP, D)
    xrows = to_experts(jax.vmap(scatter_rows)(places, xrep))
    grows = to_experts(jax.vmap(scatter_rows)(places, grep))
    gate2 = gate_w.reshape(EXPERTS, 2, D, FF // 2)
    up2 = up_w.reshape(EXPERTS, 2, D, FF // 2)
    down2 = down_w.reshape(EXPERTS, 2, FF // 2, D)

    def expert(item):
        r, dy, gw, uw, vw = item
        q0 = backward_half(r, dy, gw[0], uw[0], vw[0]).astype(jnp.float32)
        q1 = backward_half(r, dy, gw[1], uw[1], vw[1]).astype(jnp.float32)
        return (q0 + q1).astype(jnp.bfloat16)

    outs = lax.map(expert, (xrows, grows, gate2, up2, down2))
    back = from_experts(outs)

    def combine(place, buf):
        picked = jnp.dot(place, buf, preferred_element_type=jnp.float32).reshape(TOK_DEV, TOP, D)
        return jnp.sum(picked, 1).astype(jnp.bfloat16)

    return jax.vmap(combine)(places, back).reshape(TOKENS, D)


def reference(act_a, act_b, grad_b, ids_a, ids_b, scores_a, scores_b, w_gate, w_up, w_down):
    inputs_a = jnp.roll(act_a, 1, axis=0)
    upstream = jnp.roll(grad_b, -1, axis=0)
    out_a = lax.map(section_forward, (inputs_a, ids_a, scores_a, w_gate, w_up, w_down))
    grad_in_b = lax.map(section_backward, (act_b, upstream, ids_b, scores_b, w_gate, w_up, w_down))
    return out_a, grad_in_b
```

```python
import jax
import jax.numpy as jnp
from jax import lax
from jax.sharding import PartitionSpec as P


def shift(block, axis, distance):
    count = lax.axis_size(axis)
    return lax.ppermute(block, axis, [((i - distance) % count, i) for i in range(count)])


def chip_bits(count):
    return (count // 2).bit_length() - 1


def step_bit(core, step, count):
    bits = chip_bits(count)
    return step if core == 0 else bits - 1 - step


def exchange(block, step):
    count = lax.axis_size("expert")
    route = []
    for i in range(count):
        bit = step_bit(i % 2, step, count)
        route.append((i, i ^ (2 << bit)))
    return lax.ppermute(block, "expert", route)


def swap_cores(block):
    count = lax.axis_size("expert")
    return lax.ppermute(block, "expert", [(i, i ^ 1) for i in range(count)])


def gather(block, dim):
    for step in range(chip_bits(lax.axis_size("expert")) - 1):
        block = jnp.concatenate([block, exchange(block, step)], dim)
    return block


def last_exchange(block):
    return exchange(block, chip_bits(lax.axis_size("expert")) - 1)


def spread_back(block):
    for step in reversed(range(chip_bits(lax.axis_size("expert")) - 1)):
        half = block.shape[0] // 2
        other = exchange(block[half:], step)
        block = (block[:half].astype(jnp.float32) + other.astype(jnp.float32)).astype(jnp.bfloat16)
    return block


def slots(ids, wanted, tok_rows, capacity):
    chosen = jnp.any(ids == wanted, 0, keepdims=True)
    total = ids.shape[1]
    at = jnp.arange(total, dtype=jnp.int32)
    earlier = (at[:, None] < at[None, :]) & (at[:, None] // tok_rows == at[None, :] // tok_rows)
    before = jnp.dot(
        chosen.astype(jnp.bfloat16), earlier.astype(jnp.bfloat16), preferred_element_type=jnp.float32
    ).astype(jnp.int32)
    return jnp.where(chosen, (at // tok_rows)[None, :] * capacity + before, -1)


def expert_weight(ids, weights, wanted):
    return jnp.sum(jnp.where(ids == wanted, weights, 0.0), 0, keepdims=True)


def pick(slot_of, rows_out):
    return slot_of == jnp.arange(rows_out, dtype=jnp.int32)[:, None]


def matmul(left, right):
    return jnp.dot(left, right, preferred_element_type=jnp.float32)


def contract_last(left, right):
    return lax.dot_general(left, right, (((1,), (1,)), ((), ())), preferred_element_type=jnp.float32)


def contract_first(left, right):
    return lax.dot_general(left, right, (((0,), (0,)), ((), ())), preferred_element_type=jnp.float32)


def shards(act_a, act_b, grad_b, ids_a, ids_b, scores_a, scores_b, w_gate, w_up, w_down):
    count = lax.axis_size("expert")
    experts = count // 2
    tok_rows = act_a.shape[1]
    top_count = ids_a.shape[2]
    capacity = 3 * tok_rows * top_count // (2 * experts)
    gate_w, up_w, down_w = w_gate[0, 0], w_up[0, 0], w_down[0, 0]

    me = lax.axis_index("expert")
    core = me % 2
    chip = me // 2
    last = chip_bits(count) - 1
    other_chip = jnp.where(core == 0, chip ^ (1 << step_bit(0, last, count)), chip ^ (1 << step_bit(1, last, count)))

    raw_b = gather(act_b[0], 0)
    upstream = shift(grad_b, "section", -1)[0]
    incoming = shift(act_a, "section", 1)[0]

    meta = gather(
        jnp.concatenate(
            [ids_a[0].T.astype(jnp.float32), ids_b[0].T.astype(jnp.float32), scores_a[0].T, scores_b[0].T], 0
        ),
        1,
    )
    k = top_count
    all_a, all_b = meta[:k].astype(jnp.int32), meta[k : 2 * k].astype(jnp.int32)
    weights_a = meta[2 * k : 3 * k] / jnp.sum(meta[2 * k : 3 * k], 0, keepdims=True)
    weights_b = meta[3 * k :] / jnp.sum(meta[3 * k :], 0, keepdims=True)
    held = all_a.shape[1] // tok_rows * capacity

    def places(ids):
        keep = pick(slots(ids, chip, tok_rows, capacity), held)
        give = pick(slots(ids, other_chip, tok_rows, capacity), held)
        return keep, give

    keep_a, give_a = places(all_a)
    keep_b, give_b = places(all_b)
    onehot_a = jnp.concatenate([keep_a, give_a], 0).astype(jnp.bfloat16)
    onehot_b = jnp.concatenate([keep_b, give_b], 0).astype(jnp.bfloat16)
    spread_a = jnp.concatenate(
        [
            jnp.where(keep_a, expert_weight(all_a, weights_a, chip), 0.0),
            jnp.where(give_a, expert_weight(all_a, weights_a, other_chip), 0.0),
        ],
        0,
    ).astype(jnp.bfloat16)
    scale_b = jnp.concatenate(
        [
            jnp.sum(jnp.where(keep_b, expert_weight(all_b, weights_b, chip), 0.0), 1, keepdims=True),
            jnp.sum(jnp.where(give_b, expert_weight(all_b, weights_b, other_chip), 0.0), 1, keepdims=True),
        ],
        0,
    )

    def deliver(picked):
        mine, theirs = picked[:held], picked[held:]
        got = last_exchange(theirs)
        return jnp.concatenate([mine, got, swap_cores(mine), swap_cores(got)], 0)

    rows_x = deliver(matmul(onehot_b, raw_b).astype(jnp.bfloat16))
    rows_g = deliver((matmul(onehot_b, gather(upstream, 0)) * scale_b).astype(jnp.bfloat16))
    rows_a = deliver(matmul(onehot_a, gather(incoming, 0)).astype(jnp.bfloat16))

    def give_back(part, spread):
        other = swap_cores(part[2 * held :])
        summed = (part[: 2 * held].astype(jnp.float32) + other.astype(jnp.float32)).astype(jnp.bfloat16)
        back = last_exchange(summed[held:])
        tokens = contract_first(spread, jnp.concatenate([summed[:held], back], 0)).astype(jnp.bfloat16)
        return spread_back(tokens)

    first_b, second_b = lax.optimization_barrier((matmul(rows_x, gate_w), matmul(rows_x, up_w)))
    dact = lax.optimization_barrier(contract_last(rows_g, down_w))
    sig = jax.nn.sigmoid(first_b)
    dfirst = (dact * second_b * sig * (1.0 + first_b * (1.0 - sig))).astype(jnp.bfloat16)
    dsecond = (dact * first_b * sig).astype(jnp.bfloat16)
    dfirst, dsecond = lax.optimization_barrier((dfirst, dsecond))
    part_b = (contract_last(dfirst, gate_w) + contract_last(dsecond, up_w)).astype(jnp.bfloat16)
    grad_in_b = give_back(part_b, onehot_b)

    first_a, second_a = lax.optimization_barrier((matmul(rows_a, gate_w), matmul(rows_a, up_w)))
    hidden = lax.optimization_barrier((jax.nn.silu(first_a) * second_a).astype(jnp.bfloat16))
    part_a = matmul(hidden, down_w).astype(jnp.bfloat16)
    out_a = give_back(part_a, spread_a)
    return (out_a[None], grad_in_b[None])


def solution(mesh):
    tokens = P("section", "expert", None)
    weights = P("section", "expert", None, None)
    return jax.shard_map(
        shards,
        mesh=mesh,
        in_specs=(tokens,) * 7 + (weights,) * 3,
        out_specs=(tokens, tokens),
        check_vma=False,
    )
```

```python
import jax
import jax.numpy as jnp
from jax import lax
from jax.sharding import PartitionSpec as P


def shift(block, axis, distance):
    count = lax.axis_size(axis)
    return lax.ppermute(block, axis, [((i - distance) % count, i) for i in range(count)])


def chip_bits(count):
    return (count // 2).bit_length() - 1


def step_bit(core, step, count):
    bits = chip_bits(count)
    return step if core == 0 else bits - 1 - step


def exchange(block, step):
    count = lax.axis_size("expert")
    route = []
    for i in range(count):
        bit = step_bit(i % 2, step, count)
        route.append((i, i ^ (2 << bit)))
    return lax.ppermute(block, "expert", route)


def swap_cores(block):
    count = lax.axis_size("expert")
    return lax.ppermute(block, "expert", [(i, i ^ 1) for i in range(count)])


def gather(block, dim):
    for step in range(chip_bits(lax.axis_size("expert")) - 1):
        other = exchange(block, step)
        block = jnp.concatenate([block, other], dim)
    return block


def last_exchange(block):
    return exchange(block, chip_bits(lax.axis_size("expert")) - 1)


def spread_back(block):
    for step in reversed(range(chip_bits(lax.axis_size("expert")) - 1)):
        half = block.shape[0] // 2
        other = exchange(block[half:], step)
        block = (block[:half].astype(jnp.float32) + other.astype(jnp.float32)).astype(jnp.bfloat16)
    return block


def slots(ids, wanted, tok_rows, capacity):
    chosen = jnp.any(ids == wanted, 0, keepdims=True)
    total = ids.shape[1]
    at = jnp.arange(total, dtype=jnp.int32)
    earlier = (at[:, None] < at[None, :]) & (at[:, None] // tok_rows == at[None, :] // tok_rows)
    before = jnp.dot(
        chosen.astype(jnp.bfloat16), earlier.astype(jnp.bfloat16), preferred_element_type=jnp.float32
    ).astype(jnp.int32)
    return jnp.where(chosen, (at // tok_rows)[None, :] * capacity + before, -1)


def expert_weight(ids, weights, wanted):
    return jnp.sum(jnp.where(ids == wanted, weights, 0.0), 0, keepdims=True)


def pick(slot_of, rows_out):
    return slot_of == jnp.arange(rows_out, dtype=jnp.int32)[:, None]


def matmul(left, right):
    return jnp.dot(left, right, preferred_element_type=jnp.float32)


def contract_last(left, right):
    return lax.dot_general(left, right, (((1,), (1,)), ((), ())), preferred_element_type=jnp.float32)


def contract_first(left, right):
    return lax.dot_general(left, right, (((0,), (0,)), ((), ())), preferred_element_type=jnp.float32)


PARTS = {"x": 1, "g": 2, "a": 2, "rb": 2, "ra": 2}


def pieces(block, count):
    size = block.shape[-1] // count
    return [block[..., c * size : (c + 1) * size] for c in range(count)]


def shards(act_a, act_b, grad_b, ids_a, ids_b, scores_a, scores_b, w_gate, w_up, w_down):
    count = lax.axis_size("expert")
    experts = count // 2
    tok_rows = act_a.shape[1]
    top_count = ids_a.shape[2]
    capacity = 3 * tok_rows * top_count // (2 * experts)
    gate_w, up_w, down_w = w_gate[0, 0], w_up[0, 0], w_down[0, 0]

    me = lax.axis_index("expert")
    core = me % 2
    chip = me // 2
    last = chip_bits(count) - 1
    other_chip = jnp.where(core == 0, chip ^ (1 << step_bit(0, last, count)), chip ^ (1 << step_bit(1, last, count)))

    width = act_a.shape[2]

    upstream = []
    for x in pieces(grad_b, PARTS["g"]):
        upstream.append(shift(x, "section", -1)[0])
    raw_b = [gather(x, 0) for x in pieces(act_b[0], PARTS["x"])]
    incoming = []
    for x in pieces(act_a, PARTS["a"]):
        incoming.append(shift(x, "section", 1)[0])

    meta = gather(
        jnp.concatenate(
            [ids_a[0].T.astype(jnp.float32), ids_b[0].T.astype(jnp.float32), scores_a[0].T, scores_b[0].T], 0
        ),
        1,
    )
    k = top_count
    all_a, all_b = meta[:k].astype(jnp.int32), meta[k : 2 * k].astype(jnp.int32)
    weights_a = meta[2 * k : 3 * k] / jnp.sum(meta[2 * k : 3 * k], 0, keepdims=True)
    weights_b = meta[3 * k :] / jnp.sum(meta[3 * k :], 0, keepdims=True)
    held = all_a.shape[1] // tok_rows * capacity

    def places(ids):
        keep = pick(slots(ids, chip, tok_rows, capacity), held)
        give = pick(slots(ids, other_chip, tok_rows, capacity), held)
        return keep, give

    keep_a, give_a = places(all_a)
    keep_b, give_b = places(all_b)
    onehot_a = jnp.concatenate([keep_a, give_a], 0).astype(jnp.bfloat16)
    onehot_b = jnp.concatenate([keep_b, give_b], 0).astype(jnp.bfloat16)
    spread_a = jnp.concatenate(
        [
            jnp.where(keep_a, expert_weight(all_a, weights_a, chip), 0.0),
            jnp.where(give_a, expert_weight(all_a, weights_a, other_chip), 0.0),
        ],
        0,
    ).astype(jnp.bfloat16)
    scale_b = jnp.concatenate(
        [
            jnp.sum(jnp.where(keep_b, expert_weight(all_b, weights_b, chip), 0.0), 1, keepdims=True),
            jnp.sum(jnp.where(give_b, expert_weight(all_b, weights_b, other_chip), 0.0), 1, keepdims=True),
        ],
        0,
    )

    def deliver(raw, onehot, scale=None):
        out = []
        for x in raw:
            picked = matmul(onehot, x)
            picked = (picked if scale is None else picked * scale).astype(jnp.bfloat16)
            mine, theirs = picked[:held], picked[held:]
            got = last_exchange(theirs)
            mine_there = swap_cores(mine)
            got_there = swap_cores(got)
            out.append(jnp.concatenate([mine, got, mine_there, got_there], 0))
        return out

    rows_x = deliver(raw_b, onehot_b)
    rows_g = deliver([gather(x, 0) for x in upstream], onehot_b, scale_b)
    rows_a = deliver([gather(x, 0) for x in incoming], onehot_a)

    def give_back(parts, spread):
        out = []
        for part in parts:
            other = swap_cores(part[2 * held :])
            summed = (part[: 2 * held].astype(jnp.float32) + other.astype(jnp.float32)).astype(jnp.bfloat16)
            back = last_exchange(summed[held:])
            tokens = contract_first(spread, jnp.concatenate([summed[:held], back], 0)).astype(jnp.bfloat16)
            out.append(spread_back(tokens))
        return jnp.concatenate(out, 1)

    def up(rows, weight):
        total, size = 0.0, width // len(rows)
        for c, x in enumerate(rows):
            total = matmul(x, weight[c * size : (c + 1) * size]) + total
        return total

    first_b, second_b = lax.optimization_barrier((up(rows_x, gate_w), up(rows_x, up_w)))
    dact, size = 0.0, width // len(rows_g)
    for c, x in enumerate(rows_g):
        dact = contract_last(x, down_w[:, c * size : (c + 1) * size]) + dact
    dact = lax.optimization_barrier(dact)
    sig = jax.nn.sigmoid(first_b)
    dfirst = (dact * second_b * sig * (1.0 + first_b * (1.0 - sig))).astype(jnp.bfloat16)
    dsecond = (dact * first_b * sig).astype(jnp.bfloat16)
    dfirst, dsecond = lax.optimization_barrier((dfirst, dsecond))
    parts_b, size = [], width // PARTS["rb"]
    for c in range(PARTS["rb"]):
        part = contract_last(dfirst, gate_w[c * size : (c + 1) * size])
        parts_b.append((part + contract_last(dsecond, up_w[c * size : (c + 1) * size])).astype(jnp.bfloat16))
    grad_in_b = give_back(parts_b, onehot_b)

    first_a, second_a = lax.optimization_barrier((up(rows_a, gate_w), up(rows_a, up_w)))
    hidden = lax.optimization_barrier((jax.nn.silu(first_a) * second_a).astype(jnp.bfloat16))
    parts_a, size = [], width // PARTS["ra"]
    for c in range(PARTS["ra"]):
        parts_a.append(matmul(hidden, down_w[:, c * size : (c + 1) * size]).astype(jnp.bfloat16))
    out_a = give_back(parts_a, spread_a)
    return (out_a[None], grad_in_b[None])


def solution(mesh):
    tokens = P("section", "expert", None)
    weights = P("section", "expert", None, None)
    return jax.shard_map(
        shards,
        mesh=mesh,
        in_specs=(tokens,) * 7 + (weights,) * 3,
        out_specs=(tokens, tokens),
        check_vma=False,
    )
```

```python
import jax
import jax.numpy as jnp
from jax import lax
from jax.sharding import PartitionSpec as P


def shift(block, axis, distance):
    count = lax.axis_size(axis)
    return lax.ppermute(block, axis, [((i - distance) % count, i) for i in range(count)])


def chip_bits(count):
    return (count // 2).bit_length() - 1


def step_bit(core, step, count):
    bits = chip_bits(count)
    return step if core == 0 else bits - 1 - step


def exchange(block, step):
    count = lax.axis_size("expert")
    route = []
    for i in range(count):
        bit = step_bit(i % 2, step, count)
        route.append((i, i ^ (2 << bit)))
    return lax.ppermute(block, "expert", route)


def swap_cores(block):
    count = lax.axis_size("expert")
    return lax.ppermute(block, "expert", [(i, i ^ 1) for i in range(count)])


def gather(block, dim):
    for step in range(chip_bits(lax.axis_size("expert")) - 1):
        other = exchange(block, step)
        block = jnp.concatenate([block, other], dim)
    return block


def last_exchange(block):
    return exchange(block, chip_bits(lax.axis_size("expert")) - 1)


def spread_back(block):
    for step in reversed(range(chip_bits(lax.axis_size("expert")) - 1)):
        half = block.shape[0] // 2
        other = exchange(block[half:], step)
        block = (block[:half].astype(jnp.float32) + other.astype(jnp.float32)).astype(jnp.bfloat16)
    return block


def slots(ids, wanted, tok_rows, capacity):
    chosen = jnp.any(ids == wanted, 0, keepdims=True)
    total = ids.shape[1]
    at = jnp.arange(total, dtype=jnp.int32)
    earlier = (at[:, None] < at[None, :]) & (at[:, None] // tok_rows == at[None, :] // tok_rows)
    before = jnp.dot(
        chosen.astype(jnp.bfloat16), earlier.astype(jnp.bfloat16), preferred_element_type=jnp.float32
    ).astype(jnp.int32)
    return jnp.where(chosen, (at // tok_rows)[None, :] * capacity + before, -1)


def expert_weight(ids, weights, wanted):
    return jnp.sum(jnp.where(ids == wanted, weights, 0.0), 0, keepdims=True)


def pick(slot_of, rows_out):
    return slot_of == jnp.arange(rows_out, dtype=jnp.int32)[:, None]


def matmul(left, right):
    return jnp.dot(left, right, preferred_element_type=jnp.float32)


def contract_last(left, right):
    return lax.dot_general(left, right, (((1,), (1,)), ((), ())), preferred_element_type=jnp.float32)


def contract_first(left, right):
    return lax.dot_general(left, right, (((0,), (0,)), ((), ())), preferred_element_type=jnp.float32)


PARTS = {"x": 1, "g": 2, "a": 2, "rb": 2, "ra": 2}
EARLY = False


def pieces(block, count):
    size = block.shape[-1] // count
    return [block[..., c * size : (c + 1) * size] for c in range(count)]


def shards(act_a, act_b, grad_b, ids_a, ids_b, scores_a, scores_b, w_gate, w_up, w_down):
    count = lax.axis_size("expert")
    experts = count // 2
    tok_rows = act_a.shape[1]
    top_count = ids_a.shape[2]
    capacity = 3 * tok_rows * top_count // (2 * experts)
    gate_w, up_w, down_w = w_gate[0, 0], w_up[0, 0], w_down[0, 0]

    me = lax.axis_index("expert")
    core = me % 2
    chip = me // 2
    last = chip_bits(count) - 1
    other_chip = jnp.where(core == 0, chip ^ (1 << step_bit(0, last, count)), chip ^ (1 << step_bit(1, last, count)))

    width = act_a.shape[2]

    upstream = []
    for x in pieces(grad_b, PARTS["g"]):
        upstream.append(shift(x, "section", -1)[0])
    raw_b = [gather(x, 0) for x in pieces(act_b[0], PARTS["x"])]
    incoming = []
    for x in pieces(act_a, PARTS["a"]):
        incoming.append(shift(x, "section", 1)[0])

    meta = gather(
        jnp.concatenate(
            [ids_a[0].T.astype(jnp.float32), ids_b[0].T.astype(jnp.float32), scores_a[0].T, scores_b[0].T], 0
        ),
        1,
    )
    k = top_count
    all_a, all_b = meta[:k].astype(jnp.int32), meta[k : 2 * k].astype(jnp.int32)
    weights_a = meta[2 * k : 3 * k] / jnp.sum(meta[2 * k : 3 * k], 0, keepdims=True)
    weights_b = meta[3 * k :] / jnp.sum(meta[3 * k :], 0, keepdims=True)
    held = all_a.shape[1] // tok_rows * capacity

    def places(ids):
        keep = pick(slots(ids, chip, tok_rows, capacity), held)
        give = pick(slots(ids, other_chip, tok_rows, capacity), held)
        return keep, give

    keep_a, give_a = places(all_a)
    keep_b, give_b = places(all_b)
    onehot_a = jnp.concatenate([keep_a, give_a], 0).astype(jnp.bfloat16)
    onehot_b = jnp.concatenate([keep_b, give_b], 0).astype(jnp.bfloat16)
    spread_a = jnp.concatenate(
        [
            jnp.where(keep_a, expert_weight(all_a, weights_a, chip), 0.0),
            jnp.where(give_a, expert_weight(all_a, weights_a, other_chip), 0.0),
        ],
        0,
    ).astype(jnp.bfloat16)
    scale_b = jnp.concatenate(
        [
            jnp.sum(jnp.where(keep_b, expert_weight(all_b, weights_b, chip), 0.0), 1, keepdims=True),
            jnp.sum(jnp.where(give_b, expert_weight(all_b, weights_b, other_chip), 0.0), 1, keepdims=True),
        ],
        0,
    )

    def deliver(raw, onehot, name, scale=None):
        out = []
        for x in raw:
            if EARLY and name == "x":
                picked = lax.optimization_barrier(matmul(onehot[:, :tok_rows], x[:tok_rows]))
                picked = matmul(onehot[:, tok_rows:], x[tok_rows:]) + picked
            else:
                picked = matmul(onehot, x)
            picked = (picked if scale is None else picked * scale).astype(jnp.bfloat16)
            mine, theirs = picked[:held], picked[held:]
            got = last_exchange(theirs)
            mine_there = swap_cores(mine)
            got_there = swap_cores(got)
            out.append(jnp.concatenate([mine, got, mine_there, got_there], 0))
        return out

    rows_x = deliver(raw_b, onehot_b, "x")
    rows_g = deliver([gather(x, 0) for x in upstream], onehot_b, "g", scale_b)
    rows_a = deliver([gather(x, 0) for x in incoming], onehot_a, "a")

    def give_back(parts, spread):
        out = []
        for part in parts:
            other = swap_cores(part[2 * held :])
            summed = (part[: 2 * held].astype(jnp.float32) + other.astype(jnp.float32)).astype(jnp.bfloat16)
            back = last_exchange(summed[held:])
            tokens = contract_first(spread, jnp.concatenate([summed[:held], back], 0)).astype(jnp.bfloat16)
            out.append(spread_back(tokens))
        return jnp.concatenate(out, 1)

    def up(rows, weight):
        total, size = 0.0, width // len(rows)
        for c, x in enumerate(rows):
            total = matmul(x, weight[c * size : (c + 1) * size]) + total
        return total

    first_b, second_b = lax.optimization_barrier((up(rows_x, gate_w), up(rows_x, up_w)))
    dact, size = 0.0, width // len(rows_g)
    for c, x in enumerate(rows_g):
        dact = contract_last(x, down_w[:, c * size : (c + 1) * size]) + dact
    dact = lax.optimization_barrier(dact)
    sig = jax.nn.sigmoid(first_b)
    dfirst = (dact * second_b * sig * (1.0 + first_b * (1.0 - sig))).astype(jnp.bfloat16)
    dsecond = (dact * first_b * sig).astype(jnp.bfloat16)
    dfirst, dsecond = lax.optimization_barrier((dfirst, dsecond))
    parts_b, size = [], width // PARTS["rb"]
    for c in range(PARTS["rb"]):
        part = contract_last(dfirst, gate_w[c * size : (c + 1) * size])
        parts_b.append((part + contract_last(dsecond, up_w[c * size : (c + 1) * size])).astype(jnp.bfloat16))
    grad_in_b = give_back(parts_b, onehot_b)

    first_a, second_a = lax.optimization_barrier((up(rows_a, gate_w), up(rows_a, up_w)))
    hidden = lax.optimization_barrier((jax.nn.silu(first_a) * second_a).astype(jnp.bfloat16))
    parts_a, size = [], width // PARTS["ra"]
    for c in range(PARTS["ra"]):
        parts_a.append(matmul(hidden, down_w[:, c * size : (c + 1) * size]).astype(jnp.bfloat16))
    out_a = give_back(parts_a, spread_a)
    return (out_a[None], grad_in_b[None])


def solution(mesh):
    tokens = P("section", "expert", None)
    weights = P("section", "expert", None, None)
    return jax.shard_map(
        shards,
        mesh=mesh,
        in_specs=(tokens,) * 7 + (weights,) * 3,
        out_specs=(tokens, tokens),
        check_vma=False,
    )
```
